256 devices in a mesh: body: 16 (over z_hi, y), tile: 16 (over z_lo, x, core).
Axes of the slice: x: 4, y: 4, z: 8 (z_hi: 4, z_lo: 2; z = z_hi * 2 + z_lo), core: 2. Of those that a mesh axis runs over, the one named last changes fastest.
Arguments:
- panel_points: float32 [3, 131072], P(None, ('body', 'tile')), as said below
- normals: float32 [3, 131072], P(None, ('body', 'tile')), as said below
- weights: float32 [131072], P(('body', 'tile')), may hold values from 0.00024414062 to 0.0024414062
- counts: int32 [16], replicated, may hold values from 1024 to 8192, as said below
- source_points: float32 [3, 8192], replicated, as said below
- density: float32 [32, 131072], P(None, ('body', 'tile')), may hold values from -6 to 6
- incident: float32 [32, 131072], P(None, ('body', 'tile')), may hold values from -6 to 6
Outputs:
- density_next: float32 [32, 131072], P(None, ('body', 'tile'))
- amplitudes: float32 [32, 8192], P(None, 'body')
The draws below stay inside these ranges and needn't reach their ends.
Inputs may be any that keep to these rules, and one draw needn't show every extreme that they name: `counts`: one body, drawn from the seed, has exactly 8192 live panels; every other body has between 1024 and 2730. `panel_points`: panels of body b lie within distance 1.2 of a centre on a lattice of spacing 3; normals are unit vectors. `normals`: unit vectors. `source_points`: sources of body b lie within distance 0.6 of the same centre.
All inputs are finite; a program needn't handle non-finite values.
Results may differ from the reference program's by a relative error of at most 0.0044.
Values may be sent and summed in bfloat16 or wider, within the bound.
A program may use at most 64 MiB of HBM per device.

```python
import math
import jax
import jax.numpy as jnp
from jax import lax

ROWS_DEV = 512
ANGLES = 16
SOURCES = 512
BODIES = 16
CAP = 8192
N_TILE = 16


def lattice_centres(owner):
    return jnp.stack([3.0 * (owner % 4), 3.0 * (owner // 4 % 4), 3.0 * (owner // 16)], 0).astype(jnp.float32)


def unit_columns(values):
    return values / jnp.sqrt(jnp.sum(values * values, 0, keepdims=True) + 1e-06)


def surface(key):
    total = BODIES * CAP
    direction = unit_columns(jax.random.normal(jax.random.fold_in(key, 11), (3, total), jnp.float32))
    radius = jax.random.uniform(jax.random.fold_in(key, 12), (1, total), jnp.float32, 0.8, 1.2)
    owner = jnp.arange(total, dtype=jnp.int32) // CAP
    tilted = unit_columns(direction + 0.3 * jax.random.normal(jax.random.fold_in(key, 13), (3, total), jnp.float32))
    return (lattice_centres(owner) + radius * direction, tilted)


def draw_panel_points(key, part):
    return surface(key)[0]


def draw_normals(key, part):
    return surface(key)[1]


def draw_source_points(key, part):
    total = BODIES * SOURCES
    direction = unit_columns(jax.random.normal(jax.random.fold_in(key, 21), (3, total), jnp.float32))
    radius = jax.random.uniform(jax.random.fold_in(key, 22), (1, total), jnp.float32, 0.3, 0.6)
    owner = jnp.arange(total, dtype=jnp.int32) // SOURCES
    return lattice_centres(owner) + radius * direction


def draw_counts(key, part):
    largest = jax.random.randint(jax.random.fold_in(key, 31), (), 0, BODIES, jnp.int32)
    others = jax.random.randint(jax.random.fold_in(key, 32), (BODIES,), CAP // 8, CAP // 3 + 1, jnp.int32)
    return jnp.where(jnp.arange(BODIES, dtype=jnp.int32) == largest, CAP, others).astype(jnp.int32)


def level_of(rng, extent, split, low, high):
    def one(position, blocks):
        steps = jax.random.uniform(jax.random.fold_in(jax.random.fold_in(rng, 6), position), (blocks,), jnp.float32, low / len(split), high / len(split))
        return jnp.repeat(jnp.exp(steps), extent[position] // blocks).reshape((-1,) + (1,) * (len(extent) - position - 1))

    level = one(*split[0])
    for cut in split[1:]:
        level = level * one(*cut)
    return level


def gaussian(rng, extent, scale, limit, shards=(), kind=jnp.bfloat16):
    entries = jax.random.normal(rng, extent, jnp.float32) * scale
    if len(shards) > 0:
        entries = level_of(rng, extent, shards, -0.22, 0.18) * entries
    return jnp.clip(entries, min=-limit, max=limit).astype(kind)


def setup_inputs(seed: int = 0) -> dict:
    key_list = jax.random.split(jax.random.key(seed), 8)
    panel_points = draw_panel_points(jax.random.fold_in(key_list[7], 71), 0)
    normals = draw_normals(jax.random.fold_in(key_list[7], 71), 0)
    weights = jnp.clip(jnp.exp(math.log(0.0024414062) - 2.3025851 * jax.random.uniform(key_list[2], (BODIES * CAP,), jnp.float32) ** level_of(key_list[2], (BODIES * CAP,), ((0, 256),), -0.2, 0.2)), 0.00024414062, 0.0024414062)
    counts = draw_counts(jax.random.fold_in(key_list[7], 71), 0)
    source_points = draw_source_points(jax.random.fold_in(key_list[7], 71), 0)
    density = gaussian(key_list[5], (2 * ANGLES, BODIES * CAP), 1.0, 6.0, ((1, 256),), jnp.float32)
    incident = gaussian(key_list[6], (2 * ANGLES, BODIES * CAP), 1.0, 6.0, ((1, 256),), jnp.float32)
    return dict(panel_points=panel_points, normals=normals, weights=weights, counts=counts, source_points=source_points, density=density, incident=incident)


CORE_SQUARE = 0.01
WAVE = 3.0
COUPLING = 1.0

def layer_tile(targets, sources):
    offset_vec = targets[:, None, :] - sources[:3, :, None]
    radius = jnp.sqrt(lax.optimization_barrier(jnp.sum(offset_vec * offset_vec, 0)) + CORE_SQUARE)
    inverse = 1.0 / radius
    slope = lax.optimization_barrier(jnp.sum(offset_vec * sources[3:6, :, None], 0)) * inverse
    phase = WAVE * radius
    cosine = jnp.cos(phase)
    sine = jnp.sin(phase)
    scaled = sources[6][:, None] * inverse
    real = scaled * (slope * (cosine * inverse + WAVE * sine) + COUPLING * sine)
    imaginary = scaled * (slope * (sine * inverse - WAVE * cosine) - COUPLING * cosine)
    return jnp.concatenate([real, imaginary], 1).astype(jnp.bfloat16)

def point_tile(targets, sources):
    offset_vec = targets[:, None, :] - sources[:3, :, None]
    radius = jnp.sqrt(lax.optimization_barrier(jnp.sum(offset_vec * offset_vec, 0)) + CORE_SQUARE)
    scaled = sources[3][:, None] / radius
    phase = WAVE * radius
    return jnp.concatenate([scaled * jnp.cos(phase), scaled * jnp.sin(phase)], 1).astype(jnp.bfloat16)

def kernel_product(maker, dens, sources, targets, total):
    count = dens.shape[1]
    size = math.gcd(count, 1024)
    turns = count // size

    def step(turn, running):
        source_block = lax.dynamic_slice_in_dim(sources, turn * size, size, 1)
        field_block = lax.dynamic_slice_in_dim(dens, turn * size, size, 1)
        return running + jnp.dot(field_block, maker(targets, source_block), preferred_element_type=jnp.float32)
    return lax.fori_loop(0, turns, step, total)

def complex_join(product, width):
    half = product.shape[-2] // 2
    upper = product[..., :half, :]
    lower = product[..., half:, :]
    real = upper[..., :width] - lower[..., width:]
    imaginary = upper[..., width:] + lower[..., :width]
    return jnp.concatenate([real, imaginary], -2)

def reference(panel_points, normals, weights, counts, source_points, density, incident):
    channels = 2 * ANGLES
    slots = jnp.arange(BODIES * CAP, dtype=jnp.int32)
    owner = slots // CAP
    live = (slots % CAP < counts[owner]).astype(jnp.float32)
    weighted = weights * live
    geometry = jnp.concatenate([panel_points, normals, weighted[None], jnp.zeros((1, BODIES * CAP), jnp.float32)], 0)
    sigma_start = density * live
    ones_row = jnp.ones((1, BODIES * SOURCES), jnp.float32)
    source_geometry = jnp.concatenate([source_points, ones_row], 0)

    def amplitude_of(index):
        geom_body = lax.dynamic_slice_in_dim(geometry, index * CAP, CAP, 1)
        sigma_body = lax.dynamic_slice_in_dim(sigma_start, index * CAP, CAP, 1).astype(jnp.bfloat16)
        own_sources = lax.dynamic_slice_in_dim(source_points, index * SOURCES, SOURCES, 1)
        point_sources = jnp.concatenate([geom_body[:3], geom_body[6:7]], 0)
        zeros = jnp.zeros((channels, 2 * SOURCES), jnp.float32)
        raw = kernel_product(point_tile, sigma_body, point_sources, own_sources, zeros)
        return complex_join(raw, SOURCES)
    bodies_index = jnp.arange(BODIES, dtype=jnp.int32)
    stacked = lax.map(amplitude_of, bodies_index)
    amplitudes = jnp.transpose(stacked, (1, 0, 2)).reshape(channels, BODIES * SOURCES)
    source_owner = jnp.arange(BODIES * SOURCES, dtype=jnp.int32) // SOURCES

    def sweep(index):
        geom_body = lax.dynamic_slice_in_dim(geometry, index * CAP, CAP, 1)
        sigma_body = lax.dynamic_slice_in_dim(sigma_start, index * CAP, CAP, 1)
        incident_body = lax.dynamic_slice_in_dim(incident, index * CAP, CAP, 1)
        live_body = lax.dynamic_slice_in_dim(live, index * CAP, CAP, 0)
        far = jnp.where(source_owner[None, :] == index, 0.0, amplitudes).astype(jnp.bfloat16)
        block_index = jnp.arange(N_TILE, dtype=jnp.int32)

        def by_blocks(function):
            pieces = lax.map(function, block_index)
            return jnp.transpose(pieces, (1, 0, 2)).reshape(channels, CAP)

        def field_block(block):
            targets = lax.dynamic_slice_in_dim(geom_body[:3], block * ROWS_DEV, ROWS_DEV, 1)
            zeros = jnp.zeros((channels, 2 * ROWS_DEV), jnp.float32)
            return complex_join(kernel_product(point_tile, far, source_geometry, targets, zeros), ROWS_DEV)
        field = by_blocks(field_block)
        rhs = live_body * (incident_body - field)

        def operator(sigma):
            rounded = sigma.astype(jnp.bfloat16)

            def image_block(block):
                targets = lax.dynamic_slice_in_dim(geom_body[:3], block * ROWS_DEV, ROWS_DEV, 1)
                zeros = jnp.zeros((channels, 2 * ROWS_DEV), jnp.float32)
                return complex_join(kernel_product(layer_tile, rounded, geom_body, targets, zeros), ROWS_DEV)
            return by_blocks(image_block)
        sigma = sigma_body
        for sweep_step in range(2):
            sigma = live_body * (sigma + rhs - 0.5 * sigma - operator(sigma))
        return sigma
    swept = lax.map(sweep, bodies_index)
    density_next = jnp.transpose(swept, (1, 0, 2)).reshape(channels, BODIES * CAP)
    return (density_next, amplitudes)
```

```python
import functools
import math

import jax
import jax.numpy as jnp
from jax import lax
from jax.experimental import pallas as pl
from jax.experimental.pallas import tpu as pltpu
from jax.sharding import PartitionSpec as P

KAPPA = 3.0/(2*math.pi)
S3=(4.442867903030504, -7.307443421264801, 3.5947880783718604, -0.7843740306771035)
BF=jnp.bfloat16; F32=jnp.float32

def pieces(v):
    h=v.astype(BF).astype(F32); r=v-h
    m=r.astype(BF).astype(F32)
    return h,m,r-m
def pick(rows,a,b,c,d,e,f):
    z=jnp.zeros_like(rows,dtype=F32)
    for k,v in enumerate((a,b,c,d,e,f)):
        z=jnp.where(rows==k,v,z)
    return z
def dot3(a,b):
    return jnp.broadcast_to(jnp.sum(a*b,axis=0,keepdims=True),a.shape)
def target_features(x):
    h,m,l=pieces(x); a,b,c=pieces(dot3(x,x))
    rows=lax.broadcasted_iota(jnp.int32,x.shape,0)
    tail=pick(rows,a,b,c,1.0,1.0,1.0)
    return jnp.concatenate([h,h,h,m,m,l,tail,jnp.zeros_like(tail)],0).astype(BF)
def source_features(y):
    h,m,l=pieces(-2.0*y); a,b,c=pieces(dot3(y,y)+0.01*KAPPA*KAPPA)
    rows=lax.broadcasted_iota(jnp.int32,y.shape,0)
    tail=pick(rows,1.0,1.0,1.0,a,b,c)
    return jnp.concatenate([h,m,l,h,m,h,tail,jnp.zeros_like(tail)],0).astype(BF)
def normal_features(n,y):
    h,m,l=pieces(n); a,b,c=pieces(-dot3(n,y))
    rows=lax.broadcasted_iota(jnp.int32,y.shape,0)
    tail=pick(rows,0.0,0.0,0.0,a,b,c)
    return jnp.concatenate([h,m,l,h,m,h,tail,jnp.zeros_like(tail)],0).astype(BF)
def cross(a,b):
    return lax.dot_general(a,b,(((0,),(0,)),((),())),preferred_element_type=F32)
def wave(u):
    inv=lax.rsqrt(u); turn=u*inv
    f=turn-jnp.round(turn); z=f*f
    s=f*(((S3[3]*z+S3[2])*z+S3[1])*z+S3[0])
    q=s*s
    b=jnp.maximum(2.0-q,1e-30)
    return inv,1.0-q,s*(b*lax.rsqrt(b))
def point_values(u):
    inv,c,s=wave(u)
    return (c*inv).astype(BF),(s*inv).astype(BF)
def layer_values(u,p):
    inv,c,s=wave(u)
    e=p*(inv*inv); g=inv+e; h=e*(inv*(1/(2*math.pi)))
    return (c*h+s*g).astype(BF),(s*h-c*g).astype(BF)

def field_kernel(tgt,src,dens,out,feat,ubuf,kbuf,acc,*,blk):
    T=tgt.shape[1]; n=src.shape[1]//blk; half=256; nh=T//half
    feat[...]=target_features(tgt[...])
    acc[...]=jnp.zeros_like(acc)
    kbuf[...]=jnp.zeros_like(kbuf)
    def fill(i,slot):
        y=src[:,pl.ds(pl.multiple_of(i*blk,blk),blk)]
        A=source_features(y)
        for th in range(nh):
            ubuf[slot,:,th*half:(th+1)*half]=cross(A,feat[:,th*half:(th+1)*half])
    def evaluate(slot):
        for th in range(nh):
            for ch in range(blk//16):
                u=ubuf[slot,ch*16:(ch+1)*16,th*half:(th+1)*half]
                re,im=point_values(u)
                kbuf[slot,ch*16:(ch+1)*16,th*half:(th+1)*half]=re
                kbuf[slot,ch*16:(ch+1)*16,T+th*half:T+(th+1)*half]=im
    def contract(i,slot):
        d=dens[:,pl.ds(pl.multiple_of(i*blk,blk),blk)]
        acc[...]+=jnp.dot(d,kbuf[slot],preferred_element_type=F32)
    fill(0,0)
    def body(k,_):
        i=2*k
        for par in range(2):
            fill(jnp.minimum(i+par+1,n-1),1-par)
            evaluate(par)
            contract(jnp.maximum(i+par-1,0),1-par)
        return 0
    lax.fori_loop(0,n//2,body,0)
    contract(n-1,1)
    out[...]=acc[...]
def field(tgt,src,dens,blk=256):
    T=tgt.shape[1]
    return pl.pallas_call(functools.partial(field_kernel,blk=blk),out_shape=jax.ShapeDtypeStruct((32,2*T),F32),
      scratch_shapes=[pltpu.VMEM((64,T),BF),pltpu.VMEM((2,blk,T),F32),pltpu.VMEM((2,blk,2*T),BF),pltpu.VMEM((32,2*T),F32)],
      compiler_params=pltpu.CompilerParams(vmem_limit_bytes=60*2**20))(tgt,src,dens)

def layer_kernel(tgt,src,nrm,dens,out,kout,feat,ubuf,pbuf,acc,*,blk):
    T=tgt.shape[1]; n=src.shape[1]//blk; half=256; nh=T//half
    feat[...]=target_features(tgt[...])
    acc[...]=jnp.zeros_like(acc)
    def fill(i,slot):
        y=src[:,pl.ds(pl.multiple_of(i*blk,blk),blk)]
        nn=nrm[:,pl.ds(pl.multiple_of(i*blk,blk),blk)]
        A=source_features(y); N=normal_features(nn,y)
        for th in range(nh):
            ubuf[slot,:,th*half:(th+1)*half]=cross(A,feat[:,th*half:(th+1)*half])
            pbuf[slot,:,th*half:(th+1)*half]=cross(N,feat[:,th*half:(th+1)*half])
    def evaluate(i,slot):
        for th in range(nh):
            for ch in range(blk//16):
                sl=(slot,slice(ch*16,(ch+1)*16),slice(th*half,(th+1)*half))
                re,im=layer_values(ubuf[sl],pbuf[sl])
                r=pl.ds(pl.multiple_of(i*blk+ch*16,16),16)
                kout[r,th*half:(th+1)*half]=re
                kout[r,T+th*half:T+(th+1)*half]=im
    def contract(i):
        o=pl.multiple_of(i*blk,blk)
        acc[...]+=jnp.dot(dens[:,pl.ds(o,blk)],kout[pl.ds(o,blk),:],preferred_element_type=F32)
    fill(0,0)
    kout[(n-1)*blk:,:]=jnp.zeros((blk,2*T),BF)
    def body(k,_):
        i=2*k
        for par in range(2):
            fill(jnp.minimum(i+par+1,n-1),1-par)
            evaluate(i+par,par)
            j=i+par-1
            contract(jnp.where(j<0,n-1,j))
        return 0
    lax.fori_loop(0,n//2,body,0)
    contract(n-1)
    out[...]=acc[...]
def layer(tgt,src,nrm,dens,blk=256):
    T=tgt.shape[1]
    return pl.pallas_call(functools.partial(layer_kernel,blk=blk),out_shape=(jax.ShapeDtypeStruct((32,2*T),F32),jax.ShapeDtypeStruct((src.shape[1],2*T),BF)),
      scratch_shapes=[pltpu.VMEM((64,T),BF),pltpu.VMEM((2,blk,T),F32),pltpu.VMEM((2,blk,T),F32),pltpu.VMEM((32,2*T),F32)],
      compiler_params=pltpu.CompilerParams(vmem_limit_bytes=60*2**20))(tgt,src,nrm,dens)


def copy_for_each(x, axis):
    peers = lax.axis_size(axis)
    return lax.all_to_all(jnp.broadcast_to(x[None], (peers, *x.shape)), axis, 0, 0, tiled=True)


def laid_out(parts, dim):
    lengths = list(parts.shape[1:])
    lengths[dim] *= parts.shape[0]
    return jnp.moveaxis(parts, 0, dim).reshape(lengths)


def collect(x, axis, dim):
    parts = copy_for_each(x, axis)
    return laid_out(parts, dim)


def over_copies(x, axis):
    everything = copy_for_each(x, axis)
    return jnp.sum(everything, axis=0)


def complex_join(product, width):
    half = product.shape[-2] // 2
    upper = product[..., :half, :]
    lower = product[..., half:, :]
    real = upper[..., :width] - lower[..., width:]
    imaginary = upper[..., width:] + lower[..., :width]
    return jnp.concatenate([real, imaginary], -2)


def image_kernel(dens, kin, out, acc):
    i = pl.program_id(0)

    @pl.when(i == 0)
    def _():
        acc[...] = jnp.zeros_like(acc)

    acc[...] += jnp.dot(dens[...], kin[...], preferred_element_type=F32)

    @pl.when(i == pl.num_programs(0) - 1)
    def _():
        out[...] = acc[...]


def image(dens, kin):
    n, w = kin.shape
    return pl.pallas_call(
        image_kernel,
        grid=(n // 1024,),
        in_specs=[pl.BlockSpec((32, 1024), lambda i: (0, i)), pl.BlockSpec((1024, w), lambda i: (i, 0))],
        out_specs=pl.BlockSpec((32, w), lambda i: (0, 0)),
        out_shape=jax.ShapeDtypeStruct((32, w), F32),
        scratch_shapes=[pltpu.VMEM((32, w), F32)],
    )(dens, kin)


def eight(a):
    return jnp.concatenate([a, jnp.zeros((5, a.shape[1]), F32)], 0)


def per_device(panel_points, normals, weights, counts, source_points, density, incident):
    channels, rows = density.shape
    group = lax.axis_index("body")
    place = lax.axis_index("tile")
    groups = lax.axis_size("body")
    per_body = source_points.shape[1] // groups
    slots = place * rows + jnp.arange(rows, dtype=jnp.int32)
    limit = lax.dynamic_index_in_dim(counts, group, 0, keepdims=False)
    live = (slots < limit).astype(F32)
    scale = KAPPA * weights * live
    own = lax.dynamic_slice_in_dim(source_points, group * per_body, per_body, 1)
    centre = own[:, :1]
    mine = eight(KAPPA * (panel_points - centre))
    geometry = jnp.concatenate([mine, eight(3.0 * normals)], 0)
    geometry_all = collect(geometry, "tile", 1)
    sigma_start = density * live

    def loaded(sigma):
        return (scale * sigma.astype(BF).astype(F32)).astype(BF)

    first = loaded(sigma_start)
    raw_amplitude = field(eight(KAPPA * (own - centre)), mine, first)
    amplitudes = over_copies(complex_join(raw_amplitude, per_body), "tile")
    every = collect(amplitudes.astype(BF), "body", 1)
    source_owner = jnp.arange(source_points.shape[1], dtype=jnp.int32) // per_body
    far = jnp.where(source_owner[None, :] == group, jnp.zeros_like(every), every)
    raw, stored = layer(mine, geometry_all[:8], geometry_all[8:], collect(first, "tile", 1))
    raw_field = field(mine, eight(KAPPA * (source_points - centre)), far)
    rhs = live * (incident - KAPPA * complex_join(raw_field, rows))
    sigma = live * (sigma_start + rhs - 0.5 * sigma_start - complex_join(raw, rows))
    raw = image(collect(loaded(sigma), "tile", 1), stored)
    sigma = live * (sigma + rhs - 0.5 * sigma - complex_join(raw, rows))
    return (sigma, amplitudes)


def solution(mesh):
    in_specs = (
        P(None, ("body", "tile")),
        P(None, ("body", "tile")),
        P(("body", "tile")),
        P(),
        P(),
        P(None, ("body", "tile")),
        P(None, ("body", "tile")),
    )
    out_specs = (P(None, ("body", "tile")), P(None, "body"))
    return jax.shard_map(
        per_device, mesh=mesh, in_specs=in_specs, out_specs=out_specs, check_vma=False
    )
```

```python
import functools
import math

import jax
import jax.numpy as jnp
from jax import lax
from jax.experimental import pallas as pl
from jax.experimental.pallas import tpu as pltpu
from jax.sharding import PartitionSpec as P

KAPPA = 3.0/(2*math.pi)
S3=(4.442867903030504, -7.307443421264801, 3.5947880783718604, -0.7843740306771035)
BF=jnp.bfloat16; F32=jnp.float32

def pieces(v):
    h=v.astype(BF).astype(F32); r=v-h
    m=r.astype(BF).astype(F32)
    return h,m,r-m
def pick(rows,a,b,c,d,e,f):
    z=jnp.zeros_like(rows,dtype=F32)
    for k,v in enumerate((a,b,c,d,e,f)):
        z=jnp.where(rows==k,v,z)
    return z
def dot3(a,b):
    return jnp.broadcast_to(jnp.sum(a*b,axis=0,keepdims=True),a.shape)
def target_features(x):
    h,m,l=pieces(x); a,b,c=pieces(dot3(x,x))
    rows=lax.broadcasted_iota(jnp.int32,x.shape,0)
    tail=pick(rows,a,b,c,1.0,1.0,1.0)
    return jnp.concatenate([h,h,h,m,m,l,tail,jnp.zeros_like(tail)],0).astype(BF)
def source_features(y):
    h,m,l=pieces(-2.0*y); a,b,c=pieces(dot3(y,y)+0.01*KAPPA*KAPPA)
    rows=lax.broadcasted_iota(jnp.int32,y.shape,0)
    tail=pick(rows,1.0,1.0,1.0,a,b,c)
    return jnp.concatenate([h,m,l,h,m,h,tail,jnp.zeros_like(tail)],0).astype(BF)
def normal_features(n,y):
    h,m,l=pieces(n); a,b,c=pieces(-dot3(n,y))
    rows=lax.broadcasted_iota(jnp.int32,y.shape,0)
    tail=pick(rows,0.0,0.0,0.0,a,b,c)
    return jnp.concatenate([h,m,l,h,m,h,tail,jnp.zeros_like(tail)],0).astype(BF)
def cross(a,b):
    return lax.dot_general(a,b,(((0,),(0,)),((),())),preferred_element_type=F32)
def wave(u):
    inv=lax.rsqrt(u); turn=u*inv
    f=turn-jnp.round(turn); z=f*f
    s=f*(((S3[3]*z+S3[2])*z+S3[1])*z+S3[0])
    q=s*s
    b=2.0-q
    return inv,1.0-q,s*(b*lax.rsqrt(b))
def point_values(u):
    inv,c,s=wave(u)
    return (c*inv).astype(BF),(s*inv).astype(BF)
def layer_values(u,p):
    inv,c,s=wave(u)
    e=p*(inv*inv); g=inv+e; h=e*(inv*(1/(2*math.pi)))
    return (c*h+s*g).astype(BF),(s*h-c*g).astype(BF)


N = 16
ROWS = 512
HALF = 256
OWNERS = 8
FIRST = 7
KEPT = 10
STEP = 16
MESH = pl.DeviceIdType.MESH


def join(raw):
    return jnp.concatenate(
        [raw[:16, :ROWS] - raw[16:, ROWS:], raw[:16, ROWS:] + raw[16:, :ROWS]], 0
    )


def sweep_kernel(
    counts, points, normals, weights, sources, dens, inc, out, amp_out,
    geo, spots, fst, feat, ubuf, pbuf, kbuf, acc, kst, gbuf, dbuf, d1buf, abuf, part, rbuf, ampf, tile,
    sfeat, afeat, nfeat, g_s, g_r, d_s, d_r, r_s, r_r, f_s, f_r, b_s, b_r, w_s, w_r, s_s, s_r,
):
    me = lax.axis_index("tile")
    group = lax.axis_index("body")

    def send(source, target, ssem, rsem, where):
        return pltpu.make_async_remote_copy(
            src_ref=source, dst_ref=target, send_sem=ssem, recv_sem=rsem,
            device_id=where, device_id_type=MESH,
        )

    barrier = pltpu.get_barrier_semaphore()

    @pl.loop(1, N)
    def _(k):
        pl.semaphore_signal(barrier, inc=1, device_id={"tile": (me + k) % N}, device_id_type=MESH)
        pl.semaphore_signal(barrier, inc=1, device_id={"body": (group + k) % N}, device_id_type=MESH)

    rows8 = lax.broadcasted_iota(jnp.int32, (8, HALF), 0)

    def only(x, first):
        if first:
            x = pltpu.roll(x, 8 - first, 0)
        return jnp.where(rows8 < 3, x, 0.0)

    def columns(i):
        return pl.ds(pl.multiple_of(i * HALF, HALF), HALF)

    first = pl.ds(pl.multiple_of(group * ROWS, ROWS), 128)
    centre = sources[:, first][:, 0:1]
    slot_of = me * ROWS + lax.broadcasted_iota(jnp.int32, (1, ROWS), 1)
    live = jnp.where(slot_of < counts[group], 1.0, 0.0)
    scale = KAPPA * weights[...] * live
    geo[0:3, :] = KAPPA * (points[...] - centre)
    geo[3:6, :] = 3.0 * normals[...]
    geo[6:8, :] = jnp.zeros((2, ROWS), F32)
    spots[...] = jnp.zeros_like(spots)
    spots[0:3, :] = KAPPA * (sources[...] - centre)
    sigma0 = dens[...] * live

    def loaded(sigma):
        return (scale * sigma.astype(BF).astype(F32)).astype(BF)

    dbuf[me] = loaded(sigma0)

    def load_targets(part_of):
        for th in range(2):
            feat[:, th * HALF:(th + 1) * HALF] = target_features(only(part_of(th), 0))

    def fill_point(a, slot):
        for th in range(2):
            c = slice(th * HALF, (th + 1) * HALF)
            ubuf[slot, :, c] = jnp.dot(a, feat[:, c], preferred_element_type=F32)

    def evaluate_point(slot, into):
        for th in range(2):
            for ch in range(HALF // STEP):
                r = slice(ch * STEP, (ch + 1) * STEP)
                re, im = point_values(ubuf[slot, r, th * HALF:(th + 1) * HALF])
                into[slot, r, th * HALF:(th + 1) * HALF] = re
                into[slot, r, ROWS + th * HALF:ROWS + (th + 1) * HALF] = im

    def flip(x):
        return jnp.transpose(x)

    @pl.loop(0, 2 * N)
    def _(i):
        sfeat[columns(i), :] = flip(source_features(spots[:, columns(i)]))

    load_targets(lambda th: spots[:, columns(2 * group + th)])
    for h in range(2):
        fill_point(flip(source_features(only(geo[:, h * HALF:(h + 1) * HALF], 0))), h)
    for h in range(2):
        evaluate_point(h, kbuf)
    raw = jnp.dot(dbuf[me, :, :HALF], kbuf[0], preferred_element_type=F32)
    raw += jnp.dot(dbuf[me, :, HALF:], kbuf[1], preferred_element_type=F32)
    part[...] = join(raw)

    def geo_copy(k):
        return send(geo, gbuf.at[me], g_s.at[k], g_r.at[k], {"tile": (me + N - k) % N})

    def dens_copy(k):
        return send(dbuf.at[me], dbuf.at[me], d_s.at[k], d_r.at[k], {"tile": (me + N - k) % N})

    def spot(t):
        return (
            pl.ds(pl.multiple_of((t // 4) * 16, 16), 16),
            pl.ds(pl.multiple_of((t % 4) * 128, 128), 128),
        )

    def reduce_copy(k):
        peer = (me + k) % N
        at = spot(peer // 2)
        return send(part.at[at[0], at[1]], rbuf.at[k], r_s.at[k], r_r.at[k], {"tile": peer})

    gbuf[me] = geo[...]
    load_targets(lambda th: geo[:, th * HALF:(th + 1) * HALF])

    def fill_field(m, h, slot):
        other = (group + 1 + m) % N
        fill_point(sfeat[columns(2 * other + h), :], slot)

    def begin():
        pl.semaphore_wait(barrier, 2 * (N - 1))

        @pl.loop(1, N)
        def _(k):
            geo_copy(k).start()
            dens_copy(k).start()

            @pl.when((me + k) % 2 == 0)
            def _():
                reduce_copy(k).start()

    fill_field(0, 0, 0)

    @pl.loop(0, KEPT)
    def _(m):
        @pl.when(m == FIRST)
        def _():
            begin()

        fill_field(m, 1, 1)
        evaluate_point(0, fst.at[m])
        fill_field((m + 1) % (N - 1), 0, 0)
        evaluate_point(1, fst.at[m])

    def full_copy(k):
        at = spot(me // 2)
        return send(tile, ampf.at[at[0], at[1]], f_s.at[k], f_r.at[me // 2], {"tile": (me + k) % N})

    def body_copy(k):
        at = spot(me // 2)
        here = abuf.at[group, at[0], at[1]]
        return send(here, here, b_s.at[k], b_r.at[k], {"body": (group + k) % N})

    def spread_copy(k):
        at = spot(me // 2)
        here = abuf.at[:, at[0], at[1]]
        return send(here, here, w_s.at[k], w_r.at[me // 2], {"tile": (me + k) % N})

    def finish_amplitudes():
        @pl.when(me % 2 == 0)
        def _():
            at = spot(me // 2)

            @pl.loop(1, N)
            def _(k):
                reduce_copy(k).wait_recv()

            total = part[at[0], at[1]]
            for k in range(1, N):
                total = total + rbuf[k]
            tile[...] = total
            ampf[at[0], at[1]] = total
            abuf[group, at[0], at[1]] = total.astype(BF)

            @pl.loop(1, N)
            def _(k):
                body_copy(k).start()
                full_copy(k).start()

    def spread_amplitudes():
        @pl.when(me % 2 == 0)
        def _():
            @pl.loop(1, N)
            def _(k):
                body_copy(k).wait_recv()

            @pl.loop(1, N)
            def _(k):
                spread_copy(k).start()

    def prepare(j, p):
        for h in range(2):
            c = slice(h * HALF, (h + 1) * HALF)
            g = gbuf[j, :, c]
            y = only(g, 0)
            afeat[p, c, :] = flip(source_features(y))
            nfeat[p, c, :] = flip(normal_features(only(g, 3), y))

    def fill_layer(p, h, slot):
        r = slice(h * HALF, (h + 1) * HALF)
        for th in range(2):
            c = slice(th * HALF, (th + 1) * HALF)
            ubuf[slot, :, c] = jnp.dot(afeat[p, r, :], feat[:, c], preferred_element_type=F32)
            pbuf[slot, :, c] = jnp.dot(nfeat[p, r, :], feat[:, c], preferred_element_type=F32)

    def evaluate_layer(j, h):
        for th in range(2):
            for ch in range(HALF // STEP):
                at = (h, slice(ch * STEP, (ch + 1) * STEP), slice(th * HALF, (th + 1) * HALF))
                re, im = layer_values(ubuf[at], pbuf[at])
                r = slice(h * HALF + ch * STEP, h * HALF + (ch + 1) * STEP)
                kst[j, r, th * HALF:(th + 1) * HALF] = re
                kst[j, r, ROWS + th * HALF:ROWS + (th + 1) * HALF] = im
                kbuf[h, at[1], th * HALF:(th + 1) * HALF] = re
                kbuf[h, at[1], ROWS + th * HALF:ROWS + (th + 1) * HALF] = im

    def contract_layer(j, h):
        c = slice(h * HALF, (h + 1) * HALF)
        acc[...] += jnp.dot(dbuf[j, :, c], kbuf[h], preferred_element_type=F32)

    acc[...] = jnp.zeros_like(acc)
    kbuf[1] = jnp.zeros((HALF, 2 * ROWS), BF)
    prepare(me, 0)
    fill_layer(0, 0, 0)

    @pl.loop(0, N)
    def _(k):
        p = k % 2
        j = (me + k) % N
        before = (me + k - (k + N - 2) // (N - 1)) % N
        after = (me + k + 1) % N

        @pl.when(k == 3)
        def _():
            finish_amplitudes()

        @pl.when(k == 9)
        def _():
            spread_amplitudes()

        @pl.when(k < N - 1)
        def _():
            geo_copy(k + 1).wait_recv()
            dens_copy(k + 1).wait_recv()

        prepare(after, 1 - p)
        fill_layer(p, 1, 1)
        evaluate_layer(j, 0)
        contract_layer(before, 1)
        fill_layer(1 - p, 0, 0)
        evaluate_layer(j, 1)
        contract_layer(j, 0)

    contract_layer((me + N - 1) % N, 1)
    image = join(acc[...])

    @pl.loop(0, OWNERS)
    def _(o):
        @pl.when(2 * o != me)
        def _():
            at = spot(o)
            here = abuf.at[:, at[0], at[1]]
            send(here, here, w_s.at[0], w_r.at[o], {"tile": (me + 1) % N}).wait_recv()

    acc[...] = jnp.zeros_like(acc)
    kbuf[1] = jnp.zeros((HALF, 2 * ROWS), BF)

    def contract_field(m, h):
        other = (group + 1 + m) % N
        acc[...] += jnp.dot(
            abuf[other, :, h * HALF:(h + 1) * HALF], kbuf[h], preferred_element_type=F32
        )

    fill_field(KEPT, 0, 0)

    @pl.loop(KEPT, N - 1)
    def _(m):
        fill_field(m, 1, 1)
        evaluate_point(0, kbuf)
        contract_field(m - (m - KEPT + N - 2) // (N - 1), 1)
        fill_field((m + 1) % (N - 1), 0, 0)
        evaluate_point(1, kbuf)
        contract_field(m, 0)

    contract_field(N - 2, 1)

    @pl.loop(0, KEPT)
    def _(m):
        other = (group + 1 + m) % N
        for h in range(2):
            acc[...] += jnp.dot(
                abuf[other, :, h * HALF:(h + 1) * HALF], fst[m, h], preferred_element_type=F32
            )

    rhs = live * (inc[...] - KAPPA * join(acc[...]))
    sigma = live * (sigma0 + rhs - 0.5 * sigma0 - image)
    d1buf[me] = loaded(sigma)

    def next_copy(k):
        return send(d1buf.at[me], d1buf.at[me], s_s.at[k], s_r.at[k], {"tile": (me + N - k) % N})

    @pl.loop(1, N)
    def _(k):
        next_copy(k).start()

    acc[...] = jnp.dot(d1buf[me], kst[me], preferred_element_type=F32)

    @pl.loop(1, N)
    def _(k):
        j = (me + k) % N
        next_copy(k).wait_recv()
        acc[...] += jnp.dot(d1buf[j], kst[j], preferred_element_type=F32)

    out[...] = live * (sigma + rhs - 0.5 * sigma - join(acc[...]))

    @pl.loop(0, OWNERS)
    def _(o):
        @pl.when(2 * o != me)
        def _():
            at = spot(o)
            send(tile, ampf.at[at[0], at[1]], f_s.at[0], f_r.at[o], {"tile": (me + 1) % N}).wait_recv()

    amp_out[...] = ampf[...]

    @pl.loop(1, N)
    def _(k):
        geo_copy(k).wait_send()
        dens_copy(k).wait_send()
        next_copy(k).wait_send()

        @pl.when((me + k) % 2 == 0)
        def _():
            reduce_copy(k).wait_send()

        @pl.when(me % 2 == 0)
        def _():
            body_copy(k).wait_send()
            full_copy(k).wait_send()
            spread_copy(k).wait_send()


def per_device(panel_points, normals, weights, counts, source_points, density, incident):
    channels, rows = density.shape
    per_body = source_points.shape[1] // lax.axis_size("body")
    V = pltpu.VMEM
    D = pltpu.SemaphoreType.DMA
    wide = 2 * rows
    return pl.pallas_call(
        sweep_kernel,
        out_shape=(
            jax.ShapeDtypeStruct((channels, rows), F32),
            jax.ShapeDtypeStruct((channels, per_body), F32),
        ),
        in_specs=[pl.BlockSpec(memory_space=pltpu.SMEM)]
        + [pl.BlockSpec(memory_space=pltpu.VMEM)] * 6,
        out_specs=(pl.BlockSpec(memory_space=pltpu.VMEM),) * 2,
        scratch_shapes=[
            V((8, rows), F32),
            V((8, N * rows), F32),
            V((KEPT, 2, HALF, wide), BF),
            V((64, rows), BF),
            V((2, HALF, rows), F32),
            V((2, HALF, rows), F32),
            V((2, HALF, wide), BF),
            V((channels, wide), F32),
            V((N, rows, wide), BF),
            V((N, 8, rows), F32),
            V((N, channels, rows), BF),
            V((N, channels, rows), BF),
            V((N, channels, per_body), BF),
            V((channels, per_body), F32),
            V((N, 16, 128), F32),
            V((channels, per_body), F32),
            V((16, 128), F32),
            V((N * rows, 64), BF),
            V((2, rows, 64), BF),
            V((2, rows, 64), BF),
        ]
        + [D((N,))] * 14,
        compiler_params=pltpu.CompilerParams(
            collective_id=0, has_side_effects=True, vmem_limit_bytes=60 * 2**20
        ),
    )(counts, panel_points, normals, weights[None], source_points, density, incident)


def solution(mesh):
    in_specs = (
        P(None, ("body", "tile")),
        P(None, ("body", "tile")),
        P(("body", "tile")),
        P(),
        P(),
        P(None, ("body", "tile")),
        P(None, ("body", "tile")),
    )
    out_specs = (P(None, ("body", "tile")), P(None, "body"))
    return jax.shard_map(
        per_device, mesh=mesh, in_specs=in_specs, out_specs=out_specs, check_vma=False
    )
```

```python
import functools
import math

import jax
import jax.numpy as jnp
from jax import lax
from jax.experimental import pallas as pl
from jax.experimental.pallas import tpu as pltpu
from jax.sharding import PartitionSpec as P

KAPPA = 3.0/(2*math.pi)
S3=(4.442867903030504, -7.307443421264801, 3.5947880783718604, -0.7843740306771035)
BF=jnp.bfloat16; F32=jnp.float32

def pieces(v):
    h=v.astype(BF).astype(F32); r=v-h
    m=r.astype(BF).astype(F32)
    return h,m,r-m
def pick(rows,a,b,c,d,e,f):
    z=jnp.zeros_like(rows,dtype=F32)
    for k,v in enumerate((a,b,c,d,e,f)):
        z=jnp.where(rows==k,v,z)
    return z
def dot3(a,b):
    return jnp.broadcast_to(jnp.sum(a*b,axis=0,keepdims=True),a.shape)
def target_features(x):
    h,m,l=pieces(x); a,b,c=pieces(dot3(x,x))
    rows=lax.broadcasted_iota(jnp.int32,x.shape,0)
    tail=pick(rows,a,b,c,1.0,1.0,1.0)
    return jnp.concatenate([h,h,h,m,m,l,tail,jnp.zeros_like(tail)],0).astype(BF)
def source_features(y):
    h,m,l=pieces(-2.0*y); a,b,c=pieces(dot3(y,y)+0.01*KAPPA*KAPPA)
    rows=lax.broadcasted_iota(jnp.int32,y.shape,0)
    tail=pick(rows,1.0,1.0,1.0,a,b,c)
    return jnp.concatenate([h,m,l,h,m,h,tail,jnp.zeros_like(tail)],0).astype(BF)
def normal_features(n,y):
    h,m,l=pieces(n); a,b,c=pieces(-dot3(n,y))
    rows=lax.broadcasted_iota(jnp.int32,y.shape,0)
    tail=pick(rows,0.0,0.0,0.0,a,b,c)
    return jnp.concatenate([h,m,l,h,m,h,tail,jnp.zeros_like(tail)],0).astype(BF)
def cross(a,b):
    return lax.dot_general(a,b,(((0,),(0,)),((),())),preferred_element_type=F32)
def wave(u):
    inv=lax.rsqrt(u); turn=u*inv
    f=turn-jnp.round(turn); z=f*f
    s=f*(((S3[3]*z+S3[2])*z+S3[1])*z+S3[0])
    q=s*s
    b=2.0-q
    return inv,1.0-q,s*(b*lax.rsqrt(b))
def point_values(u):
    inv,c,s=wave(u)
    return (c*inv).astype(BF),(s*inv).astype(BF)
def layer_values(u,p):
    inv,c,s=wave(u)
    e=p*(inv*inv); g=inv+e; h=e*(inv*(1/(2*math.pi)))
    return (c*h+s*g).astype(BF),(s*h-c*g).astype(BF)


N = 16
ROWS = 512
HALF = 256
OWNERS = 8
FIRST = 6
KEPT = 15
STEP = 16
MESH = pl.DeviceIdType.MESH


def join(raw):
    return jnp.concatenate(
        [raw[:16, :ROWS] - raw[16:, ROWS:], raw[:16, ROWS:] + raw[16:, :ROWS]], 0
    )


def sweep_kernel(
    counts, points, normals, weights, sources, dens, inc, out, amp_out,
    geo, spots, fst, feat, ubuf, pbuf, kbuf, acc, kst, gbuf, dbuf, d1buf, abuf, part, rbuf, ampf, tile,
    sfeat, afeat, nfeat, g_s, g_r, d_s, d_r, r_s, r_r, f_s, f_r, b_s, b_r, w_s, w_r, s_s, s_r,
):
    me = lax.axis_index("tile")
    group = lax.axis_index("body")

    def send(source, target, ssem, rsem, where):
        return pltpu.make_async_remote_copy(
            src_ref=source, dst_ref=target, send_sem=ssem, recv_sem=rsem,
            device_id=where, device_id_type=MESH,
        )

    barrier = pltpu.get_barrier_semaphore()

    @pl.loop(1, N)
    def _(k):
        pl.semaphore_signal(barrier, inc=1, device_id={"tile": (me + k) % N}, device_id_type=MESH)
        pl.semaphore_signal(barrier, inc=1, device_id={"body": (group + k) % N}, device_id_type=MESH)

    rows8 = lax.broadcasted_iota(jnp.int32, (8, HALF), 0)

    def only(x, first):
        if first:
            x = pltpu.roll(x, 8 - first, 0)
        return jnp.where(rows8 < 3, x, 0.0)

    def columns(i):
        return pl.ds(pl.multiple_of(i * HALF, HALF), HALF)

    first = pl.ds(pl.multiple_of(group * ROWS, ROWS), 128)
    centre = sources[:, first][:, 0:1]
    slot_of = me * ROWS + lax.broadcasted_iota(jnp.int32, (1, ROWS), 1)
    live = jnp.where(slot_of < counts[group], 1.0, 0.0)
    scale = KAPPA * weights[...] * live
    geo[0:3, :] = KAPPA * (points[...] - centre)
    geo[3:6, :] = 3.0 * normals[...]
    geo[6:8, :] = jnp.zeros((2, ROWS), F32)
    spots[...] = jnp.zeros_like(spots)
    spots[0:3, :] = KAPPA * (sources[...] - centre)
    sigma0 = dens[...] * live

    def loaded(sigma):
        return (scale * sigma.astype(BF).astype(F32)).astype(BF)

    dbuf[me] = loaded(sigma0)

    def load_targets(part_of):
        for th in range(2):
            feat[:, th * HALF:(th + 1) * HALF] = target_features(only(part_of(th), 0))

    def fill_point(a, slot):
        for th in range(2):
            c = slice(th * HALF, (th + 1) * HALF)
            ubuf[slot, :, c] = jnp.dot(a, feat[:, c], preferred_element_type=F32)

    def evaluate_point(slot, into):
        for th in range(2):
            for ch in range(HALF // STEP):
                r = slice(ch * STEP, (ch + 1) * STEP)
                re, im = point_values(ubuf[slot, r, th * HALF:(th + 1) * HALF])
                into[slot, r, th * HALF:(th + 1) * HALF] = re
                into[slot, r, ROWS + th * HALF:ROWS + (th + 1) * HALF] = im

    def flip(x):
        return jnp.transpose(x)

    @pl.loop(0, 2 * N)
    def _(i):
        sfeat[columns(i), :] = flip(source_features(spots[:, columns(i)]))

    load_targets(lambda th: spots[:, columns(2 * group + th)])
    for h in range(2):
        fill_point(flip(source_features(only(geo[:, h * HALF:(h + 1) * HALF], 0))), h)
    for h in range(2):
        evaluate_point(h, kbuf)
    raw = jnp.dot(dbuf[me, :, :HALF], kbuf[0], preferred_element_type=F32)
    raw += jnp.dot(dbuf[me, :, HALF:], kbuf[1], preferred_element_type=F32)
    part[...] = join(raw)

    partner = me + 1 - 2 * (me % 2)
    chips = N // 2

    def to_chip(ref, ss, rs, d):
        own = ref.at[me]
        return send(own, own, ss.at[d], rs.at[d], {"tile": (me + N - 2 * d) % N})

    def to_partner(ref, ss, rs):
        own = ref.at[me]
        return send(own, own, ss.at[chips], rs.at[chips], {"tile": partner})

    def relay(ref, ss, rs, d):
        got = ref.at[(me + 2 * d) % N]
        return send(got, got, ss.at[chips + d], rs.at[chips + d], {"tile": partner})

    panels = ((gbuf, g_s, g_r), (dbuf, d_s, d_r))

    def spot(t):
        return (
            pl.ds(pl.multiple_of((t // 4) * 16, 16), 16),
            pl.ds(pl.multiple_of((t % 4) * 128, 128), 128),
        )

    def reduce_copy(k):
        peer = (me + k) % N
        at = spot(peer // 2)
        return send(part.at[at[0], at[1]], rbuf.at[k], r_s.at[k], r_r.at[k], {"tile": peer})

    gbuf[me] = geo[...]
    load_targets(lambda th: geo[:, th * HALF:(th + 1) * HALF])

    def fill_field(m, h, slot):
        other = (group + 1 + m) % N
        fill_point(sfeat[columns(2 * other + h), :], slot)

    def begin():
        pl.semaphore_wait(barrier, 2 * (N - 1))

        for buffers in panels:
            to_partner(*buffers).start()
        for d in (1, 2):
            for buffers in panels:
                to_chip(*buffers, d).start()

        @pl.loop(1, N)
        def _(k):
            @pl.when((me + k) % 2 == 0)
            def _():
                reduce_copy(k).start()

    fill_field(0, 0, 0)

    @pl.loop(0, KEPT)
    def _(m):
        @pl.when(m == FIRST)
        def _():
            begin()

        fill_field(m, 1, 1)
        evaluate_point(0, fst.at[m])
        fill_field((m + 1) % (N - 1), 0, 0)
        evaluate_point(1, fst.at[m])

    def full_copy(k):
        at = spot(me // 2)
        return send(tile, ampf.at[at[0], at[1]], f_s.at[k], f_r.at[me // 2], {"tile": (me + k) % N})

    def body_copy(k):
        here = abuf.at[me // 2, group]
        return send(here, here, b_s.at[k], b_r.at[k], {"body": (group + k) % N})

    def spread_copy(k):
        here = abuf.at[me // 2]
        return send(here, here, w_s.at[k], w_r.at[me // 2], {"tile": (me + k) % N})

    def finish_amplitudes():
        @pl.when(me % 2 == 0)
        def _():
            at = spot(me // 2)

            @pl.loop(1, N)
            def _(k):
                reduce_copy(k).wait_recv()

            total = part[at[0], at[1]]
            for k in range(1, N):
                total = total + rbuf[k]
            tile[...] = total
            ampf[at[0], at[1]] = total
            abuf[me // 2, group] = total.astype(BF)

            @pl.loop(1, N)
            def _(k):
                body_copy(k).start()
                full_copy(k).start()

    def spread_amplitudes():
        @pl.when(me % 2 == 0)
        def _():
            @pl.loop(1, N)
            def _(k):
                body_copy(k).wait_recv()

            @pl.loop(1, N)
            def _(k):
                spread_copy(k).start()

    def prepare(j, h):
        g = gbuf[j, :, h * HALF:(h + 1) * HALF]
        y = only(g, 0)
        afeat[h] = flip(source_features(y))
        nfeat[h] = flip(normal_features(only(g, 3), y))

    def fill_layer(h):
        for th in range(2):
            c = slice(th * HALF, (th + 1) * HALF)
            ubuf[h, :, c] = jnp.dot(afeat[h], feat[:, c], preferred_element_type=F32)
            pbuf[h, :, c] = jnp.dot(nfeat[h], feat[:, c], preferred_element_type=F32)

    def evaluate_layer(j, h):
        for th in range(2):
            for ch in range(HALF // STEP):
                a = slice(ch * STEP, (ch + 1) * STEP)
                c = slice(th * HALF, (th + 1) * HALF)
                d = slice(ROWS + th * HALF, ROWS + (th + 1) * HALF)
                re, im = layer_values(ubuf[h, a, c], pbuf[h, a, c])
                r = slice(h * HALF + ch * STEP, h * HALF + (ch + 1) * STEP)
                kst[j, r, c] = re
                kst[j, r, d] = im
                kbuf[h, a, c] = re
                kbuf[h, a, d] = im

    def contract_layer(j, h):
        acc[...] += jnp.dot(
            dbuf[j, :, h * HALF:(h + 1) * HALF], kbuf[h], preferred_element_type=F32
        )

    acc[...] = jnp.zeros_like(acc)
    kbuf[1] = jnp.zeros((HALF, 2 * ROWS), BF)
    prepare(me, 0)
    prepare(me, 1)
    fill_layer(0)

    @pl.loop(0, chips)
    def _(pair):
        some = (pair + chips - 1) // chips
        before = (1 - some) * me + some * ((partner + 2 * pair + N - 2) % N)
        here = ((me + 2 * pair) % N, (partner + 2 * pair) % N, (me + 2 * pair + 2) % N)

        @pl.when(pair == 0)
        def _():
            finish_amplitudes()

        @pl.when(pair == 5)
        def _():
            spread_amplitudes()

        @pl.when(pair < chips - 3)
        def _():
            for buffers in panels:
                to_chip(*buffers, pair + 3).start()

        @pl.when(pair < chips - 1)
        def _():
            for buffers in panels:
                to_chip(*buffers, pair + 1).wait_recv()
                relay(*buffers, pair + 1).start()

        @pl.when(pair == 0)
        def _():
            for buffers in panels:
                to_partner(*buffers).wait_recv()

        @pl.when(pair > 0)
        def _():
            for buffers in panels:
                relay(*buffers, pair).wait_recv()

        for t in range(4):
            h = t % 2
            fill_layer(1 - h)
            evaluate_layer(here[t // 2], h)
            prepare(here[t // 2 + 1], h)
            contract_layer(before if t == 0 else here[(t - 1) // 2], 1 - h)

    contract_layer((partner + N - 2) % N, 1)
    image = join(acc[...])

    @pl.loop(0, OWNERS)
    def _(o):
        @pl.when(2 * o != me)
        def _():
            here = abuf.at[o]
            send(here, here, w_s.at[0], w_r.at[o], {"tile": (me + 1) % N}).wait_recv()

    acc[...] = jnp.zeros_like(acc)
    def far(other, h):
        rows = [
            jnp.concatenate([abuf[c + 2 * h, other], abuf[c + 2 * h + 1, other]], 1)
            for c in (0, 4)
        ]
        return jnp.concatenate(rows, 0)

    @pl.loop(0, KEPT)
    def _(m):
        other = (group + 1 + m) % N
        raw = jnp.dot(far(other, 0), fst[m, 0], preferred_element_type=F32)
        raw += jnp.dot(far(other, 1), fst[m, 1], preferred_element_type=F32)
        acc[...] += raw

    rhs = live * (inc[...] - KAPPA * join(acc[...]))
    sigma = live * (sigma0 + rhs - 0.5 * sigma0 - image)
    d1buf[me] = loaded(sigma)

    update = (d1buf, s_s, s_r)

    @pl.loop(1, chips)
    def _(d):
        to_chip(*update, d).start()

    to_partner(*update).start()
    acc[...] = jnp.dot(d1buf[me], kst[me], preferred_element_type=F32)

    def apply(j):
        acc[...] += jnp.dot(d1buf[j], kst[j], preferred_element_type=F32)

    to_partner(*update).wait_recv()
    apply(partner)

    @pl.loop(1, chips)
    def _(d):
        to_chip(*update, d).wait_recv()
        relay(*update, d).start()
        apply((me + 2 * d) % N)

    @pl.loop(1, chips)
    def _(d):
        relay(*update, d).wait_recv()
        apply((partner + 2 * d) % N)

    out[...] = live * (sigma + rhs - 0.5 * sigma - join(acc[...]))

    @pl.loop(0, OWNERS)
    def _(o):
        @pl.when(2 * o != me)
        def _():
            at = spot(o)
            send(tile, ampf.at[at[0], at[1]], f_s.at[0], f_r.at[o], {"tile": (me + 1) % N}).wait_recv()

    amp_out[...] = ampf[...]

    for buffers in panels + (update,):
        to_partner(*buffers).wait_send()

        @pl.loop(1, chips)
        def _(d):
            to_chip(*buffers, d).wait_send()
            relay(*buffers, d).wait_send()

    @pl.loop(1, N)
    def _(k):
        @pl.when((me + k) % 2 == 0)
        def _():
            reduce_copy(k).wait_send()

        @pl.when(me % 2 == 0)
        def _():
            body_copy(k).wait_send()
            full_copy(k).wait_send()
            spread_copy(k).wait_send()


def per_device(panel_points, normals, weights, counts, source_points, density, incident):
    channels, rows = density.shape
    per_body = source_points.shape[1] // lax.axis_size("body")
    V = pltpu.VMEM
    D = pltpu.SemaphoreType.DMA
    wide = 2 * rows
    return pl.pallas_call(
        sweep_kernel,
        out_shape=(
            jax.ShapeDtypeStruct((channels, rows), F32),
            jax.ShapeDtypeStruct((channels, per_body), F32),
        ),
        in_specs=[pl.BlockSpec(memory_space=pltpu.SMEM)]
        + [pl.BlockSpec(memory_space=pltpu.VMEM)] * 6,
        out_specs=(pl.BlockSpec(memory_space=pltpu.VMEM),) * 2,
        scratch_shapes=[
            V((8, rows), F32),
            V((8, N * rows), F32),
            V((KEPT, 2, HALF, wide), BF),
            V((64, rows), BF),
            V((2, HALF, rows), F32),
            V((2, HALF, rows), F32),
            V((2, HALF, wide), BF),
            V((channels, wide), F32),
            V((N, rows, wide), BF),
            V((N, 8, rows), F32),
            V((N, channels, rows), BF),
            V((N, channels, rows), BF),
            V((OWNERS, N, 16, 128), BF),
            V((channels, per_body), F32),
            V((N, 16, 128), F32),
            V((channels, per_body), F32),
            V((16, 128), F32),
            V((N * rows, 64), BF),
            V((2, HALF, 64), BF),
            V((2, HALF, 64), BF),
        ]
        + [D((N,))] * 14,
        compiler_params=pltpu.CompilerParams(
            collective_id=0, has_side_effects=True, vmem_limit_bytes=60 * 2**20
        ),
    )(counts, panel_points, normals, weights[None], source_points, density, incident)


def solution(mesh):
    in_specs = (
        P(None, ("body", "tile")),
        P(None, ("body", "tile")),
        P(("body", "tile")),
        P(),
        P(),
        P(None, ("body", "tile")),
        P(None, ("body", "tile")),
    )
    out_specs = (P(None, ("body", "tile")), P(None, "body"))
    return jax.shard_map(
        per_device, mesh=mesh, in_specs=in_specs, out_specs=out_specs, check_vma=False
    )
```

```python
import functools
import math

import jax
import jax.numpy as jnp
from jax import lax
from jax.experimental import pallas as pl
from jax.experimental.pallas import tpu as pltpu
from jax.sharding import PartitionSpec as P

KAPPA = 3.0/(2*math.pi)
S3=(4.442867903030504, -7.307443421264801, 3.5947880783718604, -0.7843740306771035)
BF=jnp.bfloat16; F32=jnp.float32

def pieces(v):
    h=v.astype(BF).astype(F32); r=v-h
    m=r.astype(BF).astype(F32)
    return h,m,r-m
def pick(rows,a,b,c,d,e,f):
    z=jnp.zeros_like(rows,dtype=F32)
    for k,v in enumerate((a,b,c,d,e,f)):
        z=jnp.where(rows==k,v,z)
    return z
def dot3(a,b):
    return jnp.broadcast_to(jnp.sum(a*b,axis=0,keepdims=True),a.shape)
def target_features(x):
    h,m,l=pieces(x); a,b,c=pieces(dot3(x,x))
    rows=lax.broadcasted_iota(jnp.int32,x.shape,0)
    tail=pick(rows,a,b,c,1.0,1.0,1.0)
    return jnp.concatenate([h,h,h,m,m,l,tail,jnp.zeros_like(tail)],0).astype(BF)
def source_features(y):
    h,m,l=pieces(-2.0*y); a,b,c=pieces(dot3(y,y)+0.01*KAPPA*KAPPA)
    rows=lax.broadcasted_iota(jnp.int32,y.shape,0)
    tail=pick(rows,1.0,1.0,1.0,a,b,c)
    return jnp.concatenate([h,m,l,h,m,h,tail,jnp.zeros_like(tail)],0).astype(BF)
def normal_features(n,y):
    h,m,l=pieces(n); a,b,c=pieces(-dot3(n,y))
    rows=lax.broadcasted_iota(jnp.int32,y.shape,0)
    tail=pick(rows,0.0,0.0,0.0,a,b,c)
    return jnp.concatenate([h,m,l,h,m,h,tail,jnp.zeros_like(tail)],0).astype(BF)
def cross(a,b):
    return lax.dot_general(a,b,(((0,),(0,)),((),())),preferred_element_type=F32)
def wave(u):
    inv=lax.rsqrt(u); turn=u*inv
    f=turn-jnp.round(turn); z=f*f
    s=f*(((S3[3]*z+S3[2])*z+S3[1])*z+S3[0])
    q=s*s
    b=2.0-q
    return inv,1.0-q,s*(b*lax.rsqrt(b))
def point_values(u):
    inv,c,s=wave(u)
    return (c*inv).astype(BF),(s*inv).astype(BF)
def layer_values(u,p):
    inv,c,s=wave(u)
    e=p*(inv*inv); g=inv+e; h=e*(inv*(1/(2*math.pi)))
    return (c*h+s*g).astype(BF),(s*h-c*g).astype(BF)


N = 16
ROWS = 512
HALF = 256
OWNERS = 8
FIRST = 5
EARLY = 10
KEPT = 15
STEP = 16
MESH = pl.DeviceIdType.MESH


def join(raw):
    return jnp.concatenate(
        [raw[:16, :ROWS] - raw[16:, ROWS:], raw[:16, ROWS:] + raw[16:, :ROWS]], 0
    )


def sweep_kernel(
    counts, points, normals, weights, sources, dens, inc, out, amp_out,
    geo, spots, fst, feat, ubuf, pbuf, kbuf, acc, kst, gbuf, dbuf, d1buf, abuf, part, rbuf, ampf, tile,
    sfeat, afeat, nfeat, g_s, g_r, d_s, d_r, r_s, r_r, f_s, f_r, b_s, b_r, w_s, w_r, s_s, s_r,
):
    me = lax.axis_index("tile")
    group = lax.axis_index("body")

    def send(source, target, ssem, rsem, where):
        return pltpu.make_async_remote_copy(
            src_ref=source, dst_ref=target, send_sem=ssem, recv_sem=rsem,
            device_id=where, device_id_type=MESH,
        )

    barrier = pltpu.get_barrier_semaphore()

    @pl.loop(1, N)
    def _(k):
        pl.semaphore_signal(barrier, inc=1, device_id={"tile": (me + k) % N}, device_id_type=MESH)
        pl.semaphore_signal(barrier, inc=1, device_id={"body": (group + k) % N}, device_id_type=MESH)

    rows8 = lax.broadcasted_iota(jnp.int32, (8, HALF), 0)

    def only(x, first):
        if first:
            x = pltpu.roll(x, 8 - first, 0)
        return jnp.where(rows8 < 3, x, 0.0)

    def columns(i):
        return pl.ds(pl.multiple_of(i * HALF, HALF), HALF)

    first = pl.ds(pl.multiple_of(group * ROWS, ROWS), 128)
    centre = sources[:, first][:, 0:1]
    slot_of = me * ROWS + lax.broadcasted_iota(jnp.int32, (1, ROWS), 1)
    live = jnp.where(slot_of < counts[group], 1.0, 0.0)
    scale = KAPPA * weights[...] * live
    geo[0:3, :] = KAPPA * (points[...] - centre)
    geo[3:6, :] = 3.0 * normals[...]
    geo[6:8, :] = jnp.zeros((2, ROWS), F32)
    spots[...] = jnp.zeros_like(spots)
    spots[0:3, :] = KAPPA * (sources[...] - centre)
    sigma0 = dens[...] * live

    def loaded(sigma):
        return (scale * sigma.astype(BF).astype(F32)).astype(BF)

    dbuf[me] = loaded(sigma0)

    def load_targets(part_of):
        for th in range(2):
            feat[:, th * HALF:(th + 1) * HALF] = target_features(only(part_of(th), 0))

    def fill_point(a, slot):
        for th in range(2):
            c = slice(th * HALF, (th + 1) * HALF)
            ubuf[slot, :, c] = jnp.dot(a, feat[:, c], preferred_element_type=F32)

    def evaluate_point(slot, into):
        for th in range(2):
            for ch in range(HALF // STEP):
                r = slice(ch * STEP, (ch + 1) * STEP)
                re, im = point_values(ubuf[slot, r, th * HALF:(th + 1) * HALF])
                into[slot, r, th * HALF:(th + 1) * HALF] = re
                into[slot, r, ROWS + th * HALF:ROWS + (th + 1) * HALF] = im

    def flip(x):
        return jnp.transpose(x)

    @pl.loop(0, 2 * N)
    def _(i):
        sfeat[columns(i), :] = flip(source_features(spots[:, columns(i)]))

    load_targets(lambda th: spots[:, columns(2 * group + th)])
    for h in range(2):
        fill_point(flip(source_features(only(geo[:, h * HALF:(h + 1) * HALF], 0))), h)
    for h in range(2):
        evaluate_point(h, kbuf)
    raw = jnp.dot(dbuf[me, :, :HALF], kbuf[0, :, :2 * ROWS], preferred_element_type=F32)
    raw += jnp.dot(dbuf[me, :, HALF:], kbuf[1, :, :2 * ROWS], preferred_element_type=F32)
    part[...] = join(raw)

    partner = me + 1 - 2 * (me % 2)
    chips = N // 2

    def to_chip(ref, ss, rs, d):
        own = ref.at[me]
        return send(own, own, ss.at[d], rs.at[d], {"tile": (me + N - 2 * d) % N})

    def to_partner(ref, ss, rs):
        own = ref.at[me]
        return send(own, own, ss.at[chips], rs.at[chips], {"tile": partner})

    def relay(ref, ss, rs, d):
        got = ref.at[(me + 2 * d) % N]
        return send(got, got, ss.at[chips + d], rs.at[chips + d], {"tile": partner})

    panels = ((gbuf, g_s, g_r), (dbuf, d_s, d_r))

    def spot(t):
        return (
            pl.ds(pl.multiple_of((t // 4) * 16, 16), 16),
            pl.ds(pl.multiple_of((t % 4) * 128, 128), 128),
        )

    def reduce_copy(k):
        peer = (me + k) % N
        at = spot(peer // 2)
        return send(part.at[at[0], at[1]], rbuf.at[k], r_s.at[k], r_r.at[k], {"tile": peer})

    gbuf[me] = geo[...]
    load_targets(lambda th: geo[:, th * HALF:(th + 1) * HALF])

    def fill_field(m, h, slot):
        other = (group + 1 + m) % N
        fill_point(sfeat[columns(2 * other + h), :], slot)

    def begin():
        pl.semaphore_wait(barrier, 2 * (N - 1))

        for buffers in panels:
            to_partner(*buffers).start()
        for d in (1, 2):
            for buffers in panels:
                to_chip(*buffers, d).start()

        @pl.loop(1, N)
        def _(k):
            @pl.when((me + k) % 2 == 0)
            def _():
                reduce_copy(k).start()

    def keep_field(m):
        fill_field(m, 1, 1)
        evaluate_point(0, fst.at[m])
        fill_field((m + 1) % (N - 1), 0, 0)
        evaluate_point(1, fst.at[m])

    fill_field(0, 0, 0)

    @pl.loop(0, EARLY)
    def _(m):
        @pl.when(m == FIRST)
        def _():
            begin()

        keep_field(m)

    def full_copy(k):
        at = spot(me // 2)
        return send(tile, ampf.at[at[0], at[1]], f_s.at[k], f_r.at[me // 2], {"tile": (me + k) % N})

    def body_copy(k):
        here = abuf.at[me // 2, group]
        return send(here, here, b_s.at[k], b_r.at[k], {"body": (group + k) % N})

    def spread_copy(k):
        here = abuf.at[me // 2]
        return send(here, here, w_s.at[k], w_r.at[me // 2], {"tile": (me + k) % N})

    def finish_amplitudes():
        @pl.when(me % 2 == 0)
        def _():
            at = spot(me // 2)

            @pl.loop(1, N)
            def _(k):
                reduce_copy(k).wait_recv()

            total = part[at[0], at[1]]
            for k in range(1, N):
                total = total + rbuf[k]
            tile[...] = total
            ampf[at[0], at[1]] = total
            abuf[me // 2, group] = total.astype(BF)

            @pl.loop(1, N)
            def _(k):
                body_copy(k).start()
                full_copy(k).start()

    def spread_amplitudes():
        @pl.when(me % 2 == 0)
        def _():
            @pl.loop(1, N)
            def _(k):
                body_copy(k).wait_recv()

            @pl.loop(1, N)
            def _(k):
                spread_copy(k).start()

    def prepare(j, h):
        g = gbuf[j, :, h * HALF:(h + 1) * HALF]
        y = only(g, 0)
        afeat[h] = flip(source_features(y))
        nfeat[h] = flip(normal_features(only(g, 3), y))

    def fill_layer(h):
        for th in range(2):
            c = slice(th * HALF, (th + 1) * HALF)
            ubuf[h, :, c] = jnp.dot(afeat[h], feat[:, c], preferred_element_type=F32)
            pbuf[h, :, c] = jnp.dot(nfeat[h], feat[:, c], preferred_element_type=F32)

    def evaluate_layer(j, h):
        for th in range(2):
            for ch in range(HALF // STEP):
                a = slice(ch * STEP, (ch + 1) * STEP)
                c = slice(th * HALF, (th + 1) * HALF)
                d = slice(ROWS + th * HALF, ROWS + (th + 1) * HALF)
                re, im = layer_values(ubuf[h, a, c], pbuf[h, a, c])
                r = slice(h * HALF + ch * STEP, h * HALF + (ch + 1) * STEP)
                kst[j, r, c] = re
                kst[j, r, d] = im
                kbuf[h, a, c] = re
                kbuf[h, a, d] = im

    def contract_layer(j, h):
        acc[...] += jnp.dot(
            dbuf[j, :, h * HALF:(h + 1) * HALF], kbuf[h, :, :2 * ROWS], preferred_element_type=F32
        )

    acc[...] = jnp.zeros_like(acc)
    kbuf[1] = jnp.zeros((HALF, 2 * ROWS + 128), BF)
    prepare(me, 0)
    prepare(me, 1)
    fill_layer(0)

    @pl.loop(0, chips)
    def _(pair):
        some = (pair + chips - 1) // chips
        before = (1 - some) * me + some * ((partner + 2 * pair + N - 2) % N)
        here = ((me + 2 * pair) % N, (partner + 2 * pair) % N, (me + 2 * pair + 2) % N)

        @pl.when(pair == 1)
        def _():
            finish_amplitudes()

        @pl.when(pair == 5)
        def _():
            spread_amplitudes()

        @pl.when(pair < chips - 3)
        def _():
            for buffers in panels:
                to_chip(*buffers, pair + 3).start()

        @pl.when(pair < chips - 1)
        def _():
            for buffers in panels:
                to_chip(*buffers, pair + 1).wait_recv()
                relay(*buffers, pair + 1).start()

        @pl.when(pair == 0)
        def _():
            for buffers in panels:
                to_partner(*buffers).wait_recv()

        @pl.when(pair > 0)
        def _():
            for buffers in panels:
                relay(*buffers, pair).wait_recv()

        for t in range(4):
            h = t % 2
            fill_layer(1 - h)
            evaluate_layer(here[t // 2], h)
            prepare(here[t // 2 + 1], h)
            contract_layer(before if t == 0 else here[(t - 1) // 2], 1 - h)

    contract_layer((partner + N - 2) % N, 1)
    image = join(acc[...])
    fill_field(EARLY, 0, 0)

    @pl.loop(EARLY, KEPT)
    def _(m):
        keep_field(m)


    @pl.loop(0, OWNERS)
    def _(o):
        @pl.when(2 * o != me)
        def _():
            here = abuf.at[o]
            send(here, here, w_s.at[0], w_r.at[o], {"tile": (me + 1) % N}).wait_recv()

    acc[...] = jnp.zeros_like(acc)
    def far(other, h):
        rows = [
            jnp.concatenate([abuf[c + 2 * h, other], abuf[c + 2 * h + 1, other]], 1)
            for c in (0, 4)
        ]
        return jnp.concatenate(rows, 0)

    @pl.loop(0, KEPT)
    def _(m):
        other = (group + 1 + m) % N
        raw = jnp.dot(far(other, 0), fst[m, 0, :, :2 * ROWS], preferred_element_type=F32)
        raw += jnp.dot(far(other, 1), fst[m, 1, :, :2 * ROWS], preferred_element_type=F32)
        acc[...] += raw

    rhs = live * (inc[...] - KAPPA * join(acc[...]))
    sigma = live * (sigma0 + rhs - 0.5 * sigma0 - image)
    d1buf[me] = loaded(sigma)

    update = (d1buf, s_s, s_r)

    to_partner(*update).start()

    @pl.loop(1, chips)
    def _(d):
        to_chip(*update, d).start()

    acc[...] = jnp.dot(d1buf[me], kst[me, :, :2 * ROWS], preferred_element_type=F32)

    def apply(j):
        acc[...] += jnp.dot(d1buf[j], kst[j, :, :2 * ROWS], preferred_element_type=F32)

    to_partner(*update).wait_recv()
    apply(partner)

    @pl.loop(1, chips)
    def _(d):
        to_chip(*update, d).wait_recv()
        relay(*update, d).start()
        apply((me + 2 * d) % N)

    @pl.loop(1, chips)
    def _(d):
        relay(*update, d).wait_recv()
        apply((partner + 2 * d) % N)

    out[...] = live * (sigma + rhs - 0.5 * sigma - join(acc[...]))

    @pl.loop(0, OWNERS)
    def _(o):
        @pl.when(2 * o != me)
        def _():
            at = spot(o)
            send(tile, ampf.at[at[0], at[1]], f_s.at[0], f_r.at[o], {"tile": (me + 1) % N}).wait_recv()

    amp_out[...] = ampf[...]

    for buffers in panels + (update,):
        to_partner(*buffers).wait_send()

        @pl.loop(1, chips)
        def _(d):
            to_chip(*buffers, d).wait_send()
            relay(*buffers, d).wait_send()

    @pl.loop(1, N)
    def _(k):
        @pl.when((me + k) % 2 == 0)
        def _():
            reduce_copy(k).wait_send()

        @pl.when(me % 2 == 0)
        def _():
            body_copy(k).wait_send()
            full_copy(k).wait_send()
            spread_copy(k).wait_send()


def per_device(panel_points, normals, weights, counts, source_points, density, incident):
    channels, rows = density.shape
    per_body = source_points.shape[1] // lax.axis_size("body")
    V = pltpu.VMEM
    D = pltpu.SemaphoreType.DMA
    wide = 2 * rows
    return pl.pallas_call(
        sweep_kernel,
        out_shape=(
            jax.ShapeDtypeStruct((channels, rows), F32),
            jax.ShapeDtypeStruct((channels, per_body), F32),
        ),
        in_specs=[pl.BlockSpec(memory_space=pltpu.SMEM)]
        + [pl.BlockSpec(memory_space=pltpu.VMEM)] * 6,
        out_specs=(pl.BlockSpec(memory_space=pltpu.VMEM),) * 2,
        scratch_shapes=[
            V((8, rows), F32),
            V((8, N * rows), F32),
            V((KEPT, 2, HALF, wide + 128), BF),
            V((64, rows), BF),
            V((2, HALF, rows + 128), F32),
            V((2, HALF, rows + 128), F32),
            V((2, HALF, wide + 128), BF),
            V((channels, wide), F32),
            V((N, rows, wide + 128), BF),
            V((N, 8, rows), F32),
            V((N, channels, rows), BF),
            V((N, channels, rows), BF),
            V((OWNERS, N, 16, 128), BF),
            V((channels, per_body), F32),
            V((N, 16, 128), F32),
            V((channels, per_body), F32),
            V((16, 128), F32),
            V((N * rows, 64), BF),
            V((2, HALF, 64), BF),
            V((2, HALF, 64), BF),
        ]
        + [D((N,))] * 14,
        compiler_params=pltpu.CompilerParams(
            collective_id=0, has_side_effects=True, vmem_limit_bytes=60 * 2**20
        ),
    )(counts, panel_points, normals, weights[None], source_points, density, incident)


def solution(mesh):
    in_specs = (
        P(None, ("body", "tile")),
        P(None, ("body", "tile")),
        P(("body", "tile")),
        P(),
        P(),
        P(None, ("body", "tile")),
        P(None, ("body", "tile")),
    )
    out_specs = (P(None, ("body", "tile")), P(None, "body"))
    return jax.shard_map(
        per_device, mesh=mesh, in_specs=in_specs, out_specs=out_specs, check_vma=False
    )
```
